32 devices in a mesh: groups: 2 (over y), ctx: 4 (over z), tp: 4 (over x, core).
Axes of the slice: x: 2, y: 2, z: 4, core: 2. Of those that a mesh axis runs over, the one named last changes fastest.
Arguments:
- query_matrix: bfloat16 [1024, 8192], P(('groups', 'ctx'), 'tp'), parts along dimension 0, may hold values from -20 to 20
- key_matrix: bfloat16 [1024, 1024], P(('groups', 'ctx'), 'tp'), parts along dimension 0, may hold values from -20 to 20
- value_matrix: bfloat16 [1024, 1024], P(('groups', 'ctx'), 'tp'), parts along dimension 0, may hold values from -6 to 6
- doc_ids: int32 [1024], P('groups'), parts along dimension 0, may hold values from 0 to 5, never falling along the last dimension, each value on 1 to 256 neighbouring positions
- out_weight: bfloat16 [8192, 4096], P('tp', 'ctx'), may hold values from -0.0625 to 0.0625
Outputs:
- projected: bfloat16 [1024, 4096], P(('groups', 'ctx'), 'tp'), parts along dimension 0
The draws below stay inside these ranges and needn't reach their ends.
There are 2 independent parts, one for each index of `groups`. The reference program is written for one: setup_inputs(seed, part) draws one part's arguments, and reference() takes and returns one part's arrays. A program takes and returns all parts, laid end to end along the dimension named above; an argument that names none is the same for every part. Nothing has to cross between parts.
Inputs may be any that keep to these rules, and one draw needn't show every extreme that they name: `doc_ids`: non-decreasing along the sequence; each document holds 1 to 256 tokens, one exactly 256.
All inputs are finite; a program needn't handle non-finite values.
Results may differ from the reference program's by a relative error of at most 0.015.
Values may be sent and summed in bfloat16 or wider, within the bound.
A program may use at most 64 MiB of HBM per device.

```python
import math
import jax
import jax.numpy as jnp
import numpy as np
from jax import lax

QUERY_HEAD_COUNT = 64
KEY_VALUE_HEADS = 8
HEAD_SIZE = 128
DWIN = 4096
DOCS = 6
SEQUENCE_TOKENS = 512
N_TP = 4


def draw_query_matrix(key, part):
    column_list = QUERY_HEAD_COUNT * HEAD_SIZE
    noise_key = jax.random.fold_in(key, 101)
    values = jnp.clip(1.7 * jax.random.normal(noise_key, (SEQUENCE_TOKENS, column_list)), -7.0, 7.0)
    return values.astype(jnp.bfloat16)


def draw_key_matrix(key, part):
    column_list = KEY_VALUE_HEADS * HEAD_SIZE
    noise_key = jax.random.fold_in(key, 202)
    values = jnp.clip(1.7 * jax.random.normal(noise_key, (SEQUENCE_TOKENS, column_list)), -7.0, 7.0)
    return values.astype(jnp.bfloat16)


def block_levels(key, extent, cuts, least, high):
    loudness = 1.0
    for position, shards_of in cuts:
        steps = jax.random.uniform(jax.random.fold_in(jax.random.fold_in(key, 6), position), (shards_of,), jnp.float32, least / len(cuts), high / len(cuts))
        loudness = loudness * jnp.repeat(jnp.exp(steps), extent[position] // shards_of).reshape((-1,) + (1,) * (len(extent) - 1 - position))
    return loudness


def split_up(count, total, limit, slope):
    portions = [(1 << 20) // math.isqrt(rank ** slope) + 1 for rank in range(2, count + 1)]
    surplus, holding = total - limit - (count - 1), [1] * (count - 1)
    while surplus > 0:
        free = [i for i in range(count - 1) if holding[i] < limit]
        mass, remaining = sum([portions[i] for i in free]), surplus
        for i in free:
            addition = min(limit - holding[i], max(1, remaining * portions[i] // mass), surplus)
            holding[i] = holding[i] + addition
            surplus = surplus - addition
    return np.array([limit] + holding)


def ragged_sizes(own_key, count, total, bound, lean):
    if count == 2:
        one = jax.random.randint(own_key, (), max(1, total - bound), min(bound, total - 1) + 1)
        return jnp.stack([one, total - one])
    lengths = jnp.asarray(split_up(count, total, bound, lean), jnp.int32)
    pairs = (count - 1) // 2
    giver, taker = lengths[1:1 + 2 * pairs:2], lengths[2:2 + 2 * pairs:2]
    slack = jnp.minimum(giver - 1, bound - taker)
    moved = jax.random.randint(jax.random.fold_in(own_key, 1), (pairs,), 0, 1 << 20) % (slack + 1)
    lengths = lengths.at[1:1 + 2 * pairs:2].set(giver - moved).at[2:2 + 2 * pairs:2].set(taker + moved)
    return lengths[jax.random.permutation(jax.random.fold_in(own_key, 2), count)]


def normal_values(stream_key, extent, spread, reach, cuts=(), held_as=jnp.bfloat16):
    values = spread * jax.random.normal(stream_key, extent, jnp.float32)
    if cuts:
        values = values * block_levels(stream_key, extent, cuts, -0.22, 0.18)
    return jnp.clip(values, -reach, reach).astype(held_as)


def setup_inputs(seed: int = 0, part: int = 0) -> dict:
    streams_of = jax.random.split(jax.random.key(seed), 6)
    own_keys = jax.random.split(jax.random.fold_in(streams_of[5], part), 6)
    query_matrix = draw_query_matrix(jax.random.fold_in(jax.random.fold_in(streams_of[5], part), 71), part)
    key_matrix = draw_key_matrix(jax.random.fold_in(jax.random.fold_in(streams_of[5], part), 71), part)
    value_matrix = normal_values(own_keys[2], (SEQUENCE_TOKENS, KEY_VALUE_HEADS * HEAD_SIZE), 1.0, 6.0, ((0, 4), (1, 4)))
    doc_ids = jnp.searchsorted(jnp.cumsum(ragged_sizes(own_keys[3], DOCS, SEQUENCE_TOKENS, SEQUENCE_TOKENS // 2, 0)), jnp.arange(SEQUENCE_TOKENS), side="right").astype(jnp.int32)
    out_weight = normal_values(streams_of[4], (QUERY_HEAD_COUNT * HEAD_SIZE, DWIN), (QUERY_HEAD_COUNT * HEAD_SIZE) ** -0.5, 0.0625, ((0, 4), (1, 4)))
    return dict(query_matrix=query_matrix, key_matrix=key_matrix, value_matrix=value_matrix, doc_ids=doc_ids, out_weight=out_weight)


rope_base = 1000000.0


def rotary_tables(rows, token_positions, heads):
    half_dim = HEAD_SIZE // 2
    frequency = jnp.power(jnp.float32(rope_base), -jnp.arange(half_dim, dtype=jnp.float32) * (2.0 / HEAD_SIZE))
    angles = token_positions.astype(jnp.float32)[:, None] * frequency[None, :]
    cosine = jnp.cos(angles)[:, None, :]
    sine = jnp.sin(angles)[:, None, :]
    values = rows.astype(jnp.float32).reshape(rows.shape[0], heads, HEAD_SIZE)
    first = values[..., :half_dim]
    second = values[..., half_dim:]
    turned = jnp.concatenate([first * cosine - second * sine, second * cosine + first * sine], -1)
    return turned.reshape(rows.shape[0], heads * HEAD_SIZE).astype(jnp.bfloat16)


def reference(query_matrix, key_matrix, value_matrix, doc_ids, out_weight):
    group_width = QUERY_HEAD_COUNT // KEY_VALUE_HEADS
    inverse_root = HEAD_SIZE ** -0.5
    token_positions = jnp.arange(SEQUENCE_TOKENS, dtype=jnp.int32)
    query_matrix_rot = rotary_tables(query_matrix, token_positions, QUERY_HEAD_COUNT).astype(jnp.float32).reshape(SEQUENCE_TOKENS, KEY_VALUE_HEADS, group_width, HEAD_SIZE).transpose(1, 0, 2, 3)
    every_key = rotary_tables(key_matrix, token_positions, KEY_VALUE_HEADS).astype(jnp.float32).reshape(SEQUENCE_TOKENS, KEY_VALUE_HEADS, HEAD_SIZE).transpose(1, 0, 2)
    every_value = value_matrix.astype(jnp.float32).reshape(SEQUENCE_TOKENS, KEY_VALUE_HEADS, HEAD_SIZE).transpose(1, 0, 2)
    block_rows = math.gcd(SEQUENCE_TOKENS, 512)
    block_count = SEQUENCE_TOKENS // block_rows

    def one_head(inputs):
        head_q, head_k, head_v = inputs

        def one_block(block_index):
            first_row = block_index * block_rows
            block_q = lax.dynamic_slice_in_dim(head_q, first_row, block_rows, 0)
            query_pos = first_row + jnp.arange(block_rows, dtype=jnp.int32)
            query_doc = lax.dynamic_slice_in_dim(doc_ids, first_row, block_rows, 0)
            scores = jnp.einsum("qgd,sd->gqs", block_q, head_k) * inverse_root
            allowed = ((query_doc[:, None] == doc_ids[None, :]) & (token_positions[None, :] <= query_pos[:, None]))[None]
            row_max = jnp.max(jnp.where(allowed, scores, -1e30), axis=-1, keepdims=True)
            weights = jnp.where(allowed, jnp.exp(scores - row_max), 0.0)
            totals = jnp.sum(weights, -1)
            rounded = lax.optimization_barrier(weights.astype(jnp.bfloat16)).astype(jnp.float32)
            mixed_rows = jnp.einsum("gqs,sd->qgd", rounded, head_v)
            return mixed_rows / totals.T[:, :, None]

        return lax.map(one_block, jnp.arange(block_count, dtype=jnp.int32)).reshape(SEQUENCE_TOKENS, group_width, HEAD_SIZE)

    attended = lax.map(one_head, (query_matrix_rot, every_key, every_value))
    attention = attended.transpose(1, 0, 2, 3).reshape(SEQUENCE_TOKENS, QUERY_HEAD_COUNT * HEAD_SIZE).astype(jnp.bfloat16)
    share_rows = QUERY_HEAD_COUNT * HEAD_SIZE // N_TP
    projected = jnp.zeros((SEQUENCE_TOKENS, DWIN), jnp.float32)
    for member in range(N_TP):
        partial_sum = jnp.dot(attention[:, member * share_rows:(member + 1) * share_rows],
                              out_weight[member * share_rows:(member + 1) * share_rows],
                              preferred_element_type=jnp.float32)
        projected = projected + lax.optimization_barrier(partial_sum.astype(jnp.bfloat16)).astype(jnp.float32)
    return projected.astype(jnp.bfloat16)
```

```python
import functools
import math

import jax
import jax.numpy as jnp
import numpy as np
from jax import lax
from jax.experimental import pallas as pl
from jax.experimental.pallas import tpu as pltpu
from jax.sharding import PartitionSpec as P

MESH = pl.DeviceIdType.MESH

HEAD_SIZE = 128


rope_base = 1000000.0


def rotary_tables(rows, token_positions, heads):
    half_dim = HEAD_SIZE // 2
    frequency = jnp.power(
        jnp.float32(rope_base), -jnp.arange(half_dim, dtype=jnp.float32) * (2.0 / HEAD_SIZE)
    )
    angles = token_positions.astype(jnp.float32)[:, None] * frequency[None, :]
    cosine = jnp.cos(angles)[:, None, :]
    sine = jnp.sin(angles)[:, None, :]
    values = rows.astype(jnp.float32).reshape(rows.shape[0], heads, HEAD_SIZE)
    first = values[..., :half_dim]
    second = values[..., half_dim:]
    turned = jnp.concatenate([first * cosine - second * sine, second * cosine + first * sine], -1)
    return turned.reshape(rows.shape[0], heads * HEAD_SIZE).astype(jnp.bfloat16)


def on_device(query_matrix, key_matrix, value_matrix, doc_ids, out_weight):
    ctx_index = lax.axis_index("ctx")
    tok_rows = query_matrix.shape[0]
    query_heads = query_matrix.shape[1] // HEAD_SIZE
    key_heads = key_matrix.shape[1] // HEAD_SIZE
    group_width = query_heads // key_heads
    inverse_root = HEAD_SIZE ** (-0.5)
    local_rows = jnp.arange(tok_rows, dtype=jnp.int32)
    given_pos = ctx_index * tok_rows + local_rows
    query_matrix_rot = rotary_tables(query_matrix, given_pos, query_heads)
    keys_here = rotary_tables(key_matrix, given_pos, key_heads)
    query_doc = jnp.take(doc_ids, given_pos, axis=0)
    query_four = query_matrix_rot.reshape(tok_rows, key_heads, group_width, HEAD_SIZE)

    def attend(state, block):
        key_block, value_block, doc_block, pos_block = block
        row_max, totals, accum = state
        scores = (
            jnp.einsum("qkgd,skd->kgqs", query_four, key_block, preferred_element_type=jnp.float32)
            * inverse_root
        )
        allowed = (
            (query_doc[:, None] == doc_block[None, :]) & (pos_block[None, :] <= given_pos[:, None])
        )[None, None]
        new_max = jnp.maximum(row_max, jnp.max(jnp.where(allowed, scores, -1e30), -1))
        weights = jnp.where(allowed, jnp.exp(scores - new_max[..., None]), 0.0)
        factor = jnp.exp(row_max - new_max)
        totals = totals * factor + jnp.sum(weights, -1)
        accum = accum * jnp.transpose(factor, (2, 0, 1))[..., None] + jnp.einsum(
            "kgqs,skd->qkgd",
            weights.astype(jnp.bfloat16),
            value_block,
            preferred_element_type=jnp.float32,
        )
        return (new_max, totals, accum)

    start_state = (
        jnp.full((key_heads, group_width, tok_rows), -1e30, jnp.float32),
        jnp.zeros((key_heads, group_width, tok_rows), jnp.float32),
        jnp.zeros((tok_rows, key_heads, group_width, HEAD_SIZE), jnp.float32),
    )
    key_piece = lax.all_gather(keys_here, "ctx", axis=0, tiled=True)
    value_piece = lax.all_gather(value_matrix, "ctx", axis=0, tiled=True)
    count = key_piece.shape[0]
    block_rows = math.gcd(count, 512)
    block_count = count // block_rows
    positions = jnp.arange(count, dtype=jnp.int32)
    blocks = (
        key_piece.reshape(block_count, block_rows, key_heads, HEAD_SIZE),
        value_piece.reshape(block_count, block_rows, key_heads, HEAD_SIZE),
        jnp.take(doc_ids, positions, axis=0).reshape(block_count, block_rows),
        positions.reshape(block_count, block_rows),
    )

    def step_block(inner_state, block):
        return (attend(inner_state, block), None)

    final_state, unused_out = lax.scan(step_block, start_state, blocks)
    row_max, totals, accum = final_state
    attention = (
        (accum / jnp.transpose(totals, (2, 0, 1))[..., None])
        .reshape(tok_rows, query_heads * HEAD_SIZE)
        .astype(jnp.bfloat16)
    )
    terms = jnp.dot(
        attention,
        lax.all_gather(out_weight, "ctx", axis=1, tiled=True),
        preferred_element_type=jnp.float32,
    )
    return lax.psum_scatter(terms.astype(jnp.bfloat16), "tp", scatter_dimension=1, tiled=True)


def fused_kernel(
    n, back, query_ref, key_ref, value_ref, doc_ref, table_ref, weight_ref, out_ref,
    query_in, key_in, table, docs, weight, rotated, bias, kv, gathered, total_lo, total_hi,
    partial, quarters, summed, landed,
    load_sem, weight_sem, kv_send, kv_recv, up_send, down_send, chunk_recv,
    quarter_send, quarter_recv, result_send, result_recv, store_sem,
):
    ctx = lax.axis_index("ctx")
    tp = lax.axis_index("tp")
    rows = query_ref.shape[0]
    kv_heads = key_ref.shape[1] // HEAD_SIZE
    query_heads = query_ref.shape[1] // HEAD_SIZE
    group_width = query_heads // kv_heads
    chunks = gathered.shape[1]
    chunk_width = gathered.shape[3]
    chunk_heads = chunk_width // HEAD_SIZE
    quarter = partial.shape[3]
    last = n - 1

    def remote(src, dst, send, recv, to_ctx, to_tp):
        return pltpu.make_async_remote_copy(
            src_ref=src, dst_ref=dst, send_sem=send, recv_sem=recv,
            device_id={"ctx": to_ctx, "tp": to_tp}, device_id_type=MESH,
        )

    barrier = pltpu.get_barrier_semaphore()
    for step in range(1, n * n):
        pl.semaphore_signal(
            barrier, inc=1,
            device_id={"ctx": lax.rem(ctx + step // n, n), "tp": lax.rem(tp + step % n, n)},
            device_id_type=MESH,
        )

    first_row = pl.multiple_of(ctx * rows, rows)
    loads = [
        pltpu.make_async_copy(key_ref, key_in, load_sem.at[0]),
        pltpu.make_async_copy(table_ref.at[:, pl.ds(first_row, rows)], table, load_sem.at[1]),
        pltpu.make_async_copy(doc_ref, docs, load_sem.at[2]),
        pltpu.make_async_copy(query_ref, query_in, load_sem.at[3]),
    ]
    value_loads = [
        pltpu.make_async_copy(
            value_ref.at[:, pl.ds(head * HEAD_SIZE, HEAD_SIZE)], kv.at[back, head, 1], load_sem.at[4 + head]
        )
        for head in range(kv_heads)
    ]
    weight_loads = [
        pltpu.make_async_copy(
            weight_ref.at[pl.ds(chunk * chunk_width, chunk_width)], weight.at[chunk], weight_sem.at[chunk]
        )
        for chunk in range(chunks)
    ]
    for load in loads + value_loads + weight_loads:
        load.start()

    def turn(values):
        values = values.astype(jnp.float32)
        return (values * table[0] + pltpu.roll(values, HEAD_SIZE // 2, 1) * table[1]).astype(jnp.bfloat16)

    loads[0].wait()
    loads[1].wait()
    for head in range(kv_heads):
        kv[back, head, 0] = turn(key_in[:, head * HEAD_SIZE : (head + 1) * HEAD_SIZE])
    for load in value_loads:
        load.wait()

    for slot in range(back):
        @pl.when(ctx < back - slot)
        def _():
            kv[slot] = jnp.zeros(kv.shape[1:], kv.dtype)

    pl.semaphore_wait(barrier, n * n - 1)

    def kv_copy(slot, head):
        return remote(
            kv.at[slot, head], kv.at[slot - 1, head], kv_send.at[slot, head], kv_recv.at[slot - 1, head],
            lax.rem(ctx + 1, n), tp,
        )

    def kv_sends(slot):
        return (ctx < last) & (ctx >= back - slot)

    @pl.when(ctx < last)
    def _():
        for head in range(kv_heads):
            kv_copy(back, head).start()

    loads[2].wait()
    own_docs = jnp.broadcast_to(docs[pl.ds(ctx, 1), :], (rows, rows)).astype(jnp.float32).T
    row_index = lax.broadcasted_iota(jnp.int32, (rows, rows), 0)
    column_index = lax.broadcasted_iota(jnp.int32, (rows, rows), 1)
    for slot in range(back + 1):
        block = ctx - back + slot
        their_docs = docs[pl.ds(lax.max(block, 0), 1), :].astype(jnp.float32)
        allowed = (own_docs == their_docs) & (block * rows + column_index <= ctx * rows + row_index) & (block >= 0)
        bias[slot] = jnp.where(allowed, 0.0, -1e30)

    loads[3].wait()
    for head in range(query_heads):
        rotated[head] = turn(query_in[:, head * HEAD_SIZE : (head + 1) * HEAD_SIZE])

    for slot in range(back - 1, 0, -1):
        for head in range(kv_heads):
            @pl.when(ctx >= back - slot)
            def _():
                kv_copy(slot + 1, head).wait_recv()

            @pl.when(kv_sends(slot))
            def _():
                kv_copy(slot, head).start()

    def up_copy(block, chunk):
        here = gathered.at[block, chunk]
        return remote(here, here, up_send.at[block, chunk], chunk_recv.at[block, chunk], lax.rem(ctx + 1, n), tp)

    def down_copy(block, chunk):
        here = gathered.at[block, chunk]
        return remote(here, here, down_send.at[block, chunk], chunk_recv.at[block, chunk], lax.rem(ctx + last, n), tp)

    scale = HEAD_SIZE ** (-0.5) * math.log2(math.e)
    contract = (((1,), (1,)), ((), ()))
    for head in range(query_heads):
        kv_head = head // group_width
        if head % group_width == 0:
            @pl.when(ctx >= back)
            def _():
                kv_copy(1, kv_head).wait_recv()

        scores = [
            lax.dot_general(rotated[head], kv[slot, kv_head, 0], contract, preferred_element_type=jnp.float32) * scale
            + bias[slot]
            for slot in range(back + 1)
        ]
        row_max = functools.reduce(jnp.maximum, scores).max(-1, keepdims=True)
        weights = [jnp.exp2(score - row_max) for score in scores]
        totals = sum(weights).sum(-1, keepdims=True)
        mixed = sum(
            jnp.dot(weights[slot].astype(jnp.bfloat16), kv[slot, kv_head, 1], preferred_element_type=jnp.float32)
            for slot in range(back + 1)
        )
        chunk, place = head // chunk_heads, head % chunk_heads
        gathered[ctx, chunk, :, place * HEAD_SIZE : (place + 1) * HEAD_SIZE] = (mixed / totals).astype(jnp.bfloat16)
        if place == chunk_heads - 1:
            @pl.when(ctx < last)
            def _():
                up_copy(ctx, chunk).start()

            @pl.when(ctx > 0)
            def _():
                down_copy(ctx, chunk).start()

    def quarter_copy(block, hop):
        to = lax.rem(tp + hop, n)
        return remote(
            partial.at[block, to], quarters.at[block, hop], quarter_send.at[block, hop], quarter_recv.at[block, hop],
            ctx, to,
        )

    def project(block, chunk, total):
        for hop in list(range(1, n)) + [0]:
            part = lax.rem(tp + hop, n)
            columns = pl.ds(pl.multiple_of(part * quarter, quarter), quarter)
            product = jnp.dot(
                gathered[block, chunk], weight[chunk, :, columns], preferred_element_type=jnp.float32
            )
            if chunk > 0:
                product = product + total[hop]
            if chunk < chunks - 1:
                total[hop] = product
            else:
                partial[block, part] = product.astype(jnp.bfloat16)
                if hop:
                    quarter_copy(block, hop).start()

    def result_copy(block):
        return remote(
            summed.at[block], landed.at[tp], result_send.at[block], result_recv.at[tp], block, ctx
        )

    def finish(block):
        value = partial[block, tp].astype(jnp.float32)
        for hop in range(1, n):
            quarter_copy(block, hop).wait_recv()
            value = value + quarters[block, hop].astype(jnp.float32)
        value = value.astype(jnp.bfloat16)
        mine = (block == ctx) & (tp == ctx)

        @pl.when(mine)
        def _():
            landed[tp] = value

        @pl.when(jnp.logical_not(mine))
        def _():
            summed[block] = value
            result_copy(block).start()

    for load in weight_loads:
        load.wait()
    for chunk in range(chunks):
        project(ctx, chunk, total_lo)

    def finish_pair(step):
        @pl.when(ctx - step >= 0)
        def _():
            finish(lax.max(ctx - step, 0))

        @pl.when((ctx + step <= last) & (step > 0))
        def _():
            finish(lax.min(ctx + step, last))

    def gather_step(step, carry):
        low, high = lax.max(ctx - step, 0), lax.min(ctx + step, last)
        has_low, has_high = ctx - step >= 0, ctx + step <= last
        for chunk in range(chunks):
            @pl.when(has_low)
            def _():
                up_copy(low, chunk).wait_recv()

                @pl.when(ctx < last)
                def _():
                    up_copy(low, chunk).start()

            @pl.when(has_high)
            def _():
                down_copy(high, chunk).wait_recv()

                @pl.when(ctx > 0)
                def _():
                    down_copy(high, chunk).start()

            @pl.when(has_low)
            def _():
                project(low, chunk, total_lo)

            @pl.when(has_high)
            def _():
                project(high, chunk, total_hi)

        finish_pair(step - 1)
        return carry

    lax.fori_loop(1, n, gather_step, 0)
    finish_pair(last)

    for part in range(n):
        @pl.when(jnp.logical_not((tp == ctx) & (tp == part)))
        def _():
            remote(
                summed.at[0], landed.at[part], result_send.at[0], result_recv.at[part], ctx, part
            ).wait_recv()

        pltpu.make_async_copy(
            landed.at[part], out_ref.at[:, pl.ds(part * quarter, quarter)], store_sem.at[part]
        ).start()

    for slot in range(1, back + 1):
        for head in range(kv_heads):
            @pl.when(kv_sends(slot))
            def _():
                kv_copy(slot, head).wait_send()

    def drain(block, carry):
        for chunk in range(chunks):
            @pl.when((block <= ctx) & (ctx < last))
            def _():
                up_copy(block, chunk).wait_send()

            @pl.when((block >= ctx) & (ctx > 0))
            def _():
                down_copy(block, chunk).wait_send()

        for hop in range(1, n):
            quarter_copy(block, hop).wait_send()

        @pl.when(jnp.logical_not((block == ctx) & (tp == ctx)))
        def _():
            result_copy(block).wait_send()

        return carry

    lax.fori_loop(0, n, drain, 0)
    for part in range(n):
        pltpu.make_async_copy(
            landed.at[part], out_ref.at[:, pl.ds(part * quarter, quarter)], store_sem.at[part]
        ).wait()


def fused(n, query_matrix, key_matrix, value_matrix, doc_ids, out_weight):
    rows, query_width = query_matrix.shape
    query_heads, kv_heads = query_width // HEAD_SIZE, key_matrix.shape[1] // HEAD_SIZE
    features = out_weight.shape[1]
    tokens = doc_ids.shape[0]
    back = -(-(tokens // 2 - 1) // rows)
    chunks = 4
    chunk_width = query_width // chunks
    quarter = features // n
    half = HEAD_SIZE // 2
    frequency = np.power(np.float32(rope_base), -np.arange(half, dtype=np.float32) * np.float32(2.0 / HEAD_SIZE))
    angles = np.arange(tokens, dtype=np.float32)[:, None] * frequency[None, :]
    cosine, sine = np.cos(angles), np.sin(angles)
    table = np.stack([np.concatenate([cosine, cosine], 1), np.concatenate([-sine, sine], 1)]).astype(np.float32)
    any_space = pl.BlockSpec(memory_space=pl.ANY)
    bf16, f32, dma = jnp.bfloat16, jnp.float32, pltpu.SemaphoreType.DMA
    return pl.pallas_call(
        functools.partial(fused_kernel, n, back),
        out_shape=jax.ShapeDtypeStruct((rows, features), bf16),
        in_specs=[any_space] * 6,
        out_specs=any_space,
        scratch_shapes=[
            pltpu.VMEM((rows, query_width), bf16),
            pltpu.VMEM((rows, kv_heads * HEAD_SIZE), bf16),
            pltpu.VMEM((2, rows, HEAD_SIZE), f32),
            pltpu.VMEM((tokens // rows, rows), jnp.int32),
            pltpu.VMEM((chunks, chunk_width, features), bf16),
            pltpu.VMEM((query_heads, rows, HEAD_SIZE), bf16),
            pltpu.VMEM((back + 1, rows, rows), f32),
            pltpu.VMEM((back + 1, kv_heads, 2, rows, HEAD_SIZE), bf16),
            pltpu.VMEM((n, chunks, rows, chunk_width), bf16),
            pltpu.VMEM((n, rows, quarter), f32),
            pltpu.VMEM((n, rows, quarter), f32),
            pltpu.VMEM((n, n, rows, quarter), bf16),
            pltpu.VMEM((n, n, rows, quarter), bf16),
            pltpu.VMEM((n, rows, quarter), bf16),
            pltpu.VMEM((n, rows, quarter), bf16),
            dma((4 + kv_heads,)),
            dma((chunks,)),
            dma((back + 1, kv_heads)),
            dma((back + 1, kv_heads)),
            dma((n, chunks)),
            dma((n, chunks)),
            dma((n, chunks)),
            dma((n, n)),
            dma((n, n)),
            dma((n,)),
            dma((n,)),
            dma((n,)),
        ],
        compiler_params=pltpu.CompilerParams(collective_id=0, has_side_effects=True),
    )(query_matrix, key_matrix, value_matrix, doc_ids.reshape(tokens // rows, rows), jnp.asarray(table), out_weight)


def solution(mesh):
    in_specs = (
        P(("groups", "ctx"), "tp"),
        P(("groups", "ctx"), "tp"),
        P(("groups", "ctx"), "tp"),
        P("groups"),
        P("tp", "ctx"),
    )
    out_specs = P(("groups", "ctx"), "tp")
    n = mesh.shape["ctx"]
    body = functools.partial(fused, n) if n == mesh.shape["tp"] else on_device
    return jax.shard_map(
        body, mesh=mesh, in_specs=in_specs, out_specs=out_specs, check_vma=False
    )
```
